16 devices in a mesh: dp: 2 (over z), vp: 8 (over y, x, core).
Axes of the slice: x: 2, y: 2, z: 2, core: 2. Of those that a mesh axis runs over, the one named last changes fastest.
Arguments:
- hidden: bfloat16 [4, 1024, 1024], P('dp')
- targets: int32 [4, 1024], P('dp')
- loss_mask: int32 [4, 1024], P('dp')
- norm_gain: float32 [1024], replicated
- emb_table: bfloat16 [152000, 1024], P('vp')
Outputs:
- output 1: float32 [], replicated
- output 2: float32 [4, 1024, 1024], P('dp')
- output 3: float32 [152000, 1024], P('vp')
- output 4: float32 [1024], replicated
All inputs are finite; a program needn't handle non-finite values.
Results may differ from the reference program's by a relative error of at most 0.001.
Values sent between devices are 32-bit elements.
A program may use at most 1 GiB of HBM per device.

```python
import math
import jax
import jax.numpy as jnp
from jax import lax

WIDTH = 1024
VOCAB_REAL = 151936
PAD_ROWS = 64
SAMPLES = 4
SEQ_LEN = 1024
ROW_BLOCK = 16
VOCAB_ROWS = VOCAB_REAL + PAD_ROWS
SOFT_CAP = 30.0
NORM_EPS = 1e-6
EMBED_STD = 23.0 / math.sqrt(WIDTH)


def draw_mask_targets(index_key):
    key_len, key_pos, key_tgt = jax.random.split(index_key, 3)
    win_len = SEQ_LEN // 2
    suffix_len = jax.random.randint(key_len, (SAMPLES,), 1, win_len + 1)
    suffix_len = suffix_len.at[0].set(win_len)
    suffix_pos = jax.random.randint(key_pos, (SAMPLES,), 0, SEQ_LEN - suffix_len + 1)
    positions = jnp.arange(SEQ_LEN)[None, :]
    inside = (positions >= suffix_pos[:, None]) & (positions < (suffix_pos + suffix_len)[:, None])
    loss_mask = inside.astype(jnp.int32)
    targets = jax.random.randint(key_tgt, (SAMPLES, SEQ_LEN), 0, VOCAB_REAL)
    return targets, loss_mask


def setup_inputs(seed: int = 0) -> dict:
    base_key = jax.random.key(seed)
    key_hid, key_gain, key_table, key_idx = jax.random.split(base_key, 4)
    hidden = jax.random.normal(key_hid, (SAMPLES, SEQ_LEN, WIDTH), jnp.float32).astype(jnp.bfloat16)
    norm_gain = 0.3 * jax.random.normal(key_gain, (WIDTH,), jnp.float32)
    emb_table = (EMBED_STD * jax.random.normal(key_table, (VOCAB_ROWS, WIDTH), jnp.float32)).astype(jnp.bfloat16)
    targets, loss_mask = draw_mask_targets(key_idx)
    return {'hidden': hidden, 'targets': targets, 'loss_mask': loss_mask, 'norm_gain': norm_gain, 'emb_table': emb_table}


def reference(hidden, targets, loss_mask, norm_gain, emb_table):
    num_blocks = SAMPLES * SEQ_LEN // ROW_BLOCK
    hid_blocks = hidden.reshape(num_blocks, ROW_BLOCK, WIDTH)
    tgt_blocks = targets.reshape(num_blocks, ROW_BLOCK)
    mask_blocks = loss_mask.reshape(num_blocks, ROW_BLOCK).astype(jnp.float32)
    mask_count = jnp.sum(mask_blocks)
    gain_vec = 1.0 + norm_gain
    col_ids = jnp.arange(VOCAB_ROWS)
    real_cols = (col_ids < VOCAB_REAL)[None, :]

    def block_step(acc_state, block_in):
        table_acc, loss_acc = acc_state
        hid_blk, tgt_blk, mask_blk = block_in
        hid_f32 = hid_blk.astype(jnp.float32)
        inv_rms = lax.rsqrt(jnp.mean(hid_f32 * hid_f32, axis=-1, keepdims=True) + NORM_EPS)
        normed = hid_f32 * inv_rms
        normed_bf = (normed * gain_vec).astype(jnp.bfloat16)
        logits = jnp.dot(normed_bf, emb_table.T, preferred_element_type=jnp.float32)
        tanh_vals = jnp.tanh(logits / SOFT_CAP)
        capped = jnp.where(real_cols, SOFT_CAP * tanh_vals, -jnp.inf)
        log_norm = jax.nn.logsumexp(capped, axis=-1)
        is_target = col_ids[None, :] == tgt_blk[:, None]
        tgt_logit = jnp.sum(jnp.where(is_target, capped, 0.0), axis=-1)
        prob_vals = jnp.exp(capped - log_norm[:, None])
        logit_grad = ((prob_vals - is_target.astype(jnp.float32)) * (1.0 - tanh_vals * tanh_vals) * (mask_blk / mask_count)[:, None]).astype(jnp.bfloat16)
        norm_grad = jnp.dot(logit_grad, emb_table, preferred_element_type=jnp.float32)
        table_acc = table_acc + jnp.dot(logit_grad.T, normed_bf, preferred_element_type=jnp.float32)
        loss_acc = loss_acc + jnp.sum((log_norm - tgt_logit) * mask_blk)
        scaled_grad = norm_grad * gain_vec
        hid_grad = inv_rms * scaled_grad - hid_f32 * (inv_rms ** 3) * jnp.mean(scaled_grad * hid_f32, axis=-1, keepdims=True)
        gain_part = jnp.sum(norm_grad * normed, axis=0)
        return (table_acc, loss_acc), (hid_grad, gain_part)

    start_state = (jnp.zeros((VOCAB_ROWS, WIDTH), jnp.float32), jnp.zeros((), jnp.float32))
    (table_grad, loss_sum), (hid_grads, gain_parts) = lax.scan(block_step, start_state, (hid_blocks, tgt_blocks, mask_blocks))
    return (loss_sum / mask_count, hid_grads.reshape(SAMPLES, SEQ_LEN, WIDTH), table_grad, jnp.sum(gain_parts, axis=0))
```

```python
import functools

import jax
import jax.numpy as jnp
from jax import lax
from jax.experimental import pallas as pl
from jax.experimental.pallas import tpu as pltpu
from jax.sharding import PartitionSpec as P

SOFT_CAP = 30.0
NORM_EPS = 1e-6
PAD_ROWS = 64
EXP_SCALE = SOFT_CAP * 1.4426950408889634
CHUNK = 256
SLOTS = 1024
NCH = SLOTS // CHUNK
MESH = pl.DeviceIdType.MESH
VMEM_LIMIT = 60 * 1024 * 1024
ANY = pl.BlockSpec(memory_space=pl.ANY)
VM = pl.BlockSpec(memory_space=pltpu.VMEM)
SM = pl.BlockSpec(memory_space=pltpu.SMEM)


def _params(**kw):
    return pltpu.CompilerParams(vmem_limit_bytes=VMEM_LIMIT, **kw)


def _prep_kernel(hid, mask, tgt, gain, u_out, half_out, hp_out, y_out, meta, hf):
    seq, width = mask.shape[1], hid.shape[1]
    pad = 16
    core = lax.rem(lax.axis_index("vp"), 2)
    iota = lax.broadcasted_iota(jnp.int32, (1, seq), 1)
    starts, lens = [], []
    for s in range(2):
        m = mask[s : s + 1, :]
        lens.append(jnp.sum(m))
        starts.append(jnp.min(jnp.where(m > 0, iota, seq)))
    len_a, len_b = lens
    start_a, start_b = starts
    n_tok = len_a + len_b
    meta[0] = start_a
    meta[1] = len_a
    meta[2] = start_b
    meta[3] = len_b
    meta[4] = n_tok
    base = [pad, pad + seq + pad]
    zeros = jnp.zeros((pad, width), jnp.float32)
    hf[0:pad] = zeros
    hf[pad + seq : 2 * pad + seq] = zeros
    hf[2 * pad + 2 * seq : 3 * pad + 2 * seq] = zeros

    def widen(i, _):
        for s in range(2):
            src = pl.multiple_of(i * 64, 64)
            hf[pl.ds(pl.multiple_of(base[s] + src, 8), 64)] = hid[
                pl.ds(s * seq + src, 64)
            ].astype(jnp.float32)
        return 0

    lax.fori_loop(0, seq // 64, widen, 0)
    pos = lax.broadcasted_iota(jnp.int32, (8, seq), 1)
    ya = pltpu.roll(jnp.broadcast_to(tgt[0:1, :], (8, seq)), lax.rem(seq - start_a, seq), 1)
    yb = pltpu.roll(
        jnp.broadcast_to(tgt[1:2, :], (8, seq)), lax.rem(len_a + seq - start_b, seq), 1
    )
    y_pack = jnp.where(pos < len_a, ya, jnp.where(pos < n_tok, yb, -1))
    for c in range(NCH):
        y_out[c] = y_pack[:, c * CHUNK : (c + 1) * CHUNK]
    gain_vec = 1.0 + gain[...]
    row8 = lax.broadcasted_iota(jnp.int32, (8, width), 0)

    def shifted(first):
        lo = pl.multiple_of((first // 8) * 8, 8)
        s = first - lo
        back = lax.rem(8 - s, 8)
        x0 = pltpu.roll(hf[pl.ds(lo, 8)], back, 0)
        x1 = pltpu.roll(hf[pl.ds(lo + 8, 8)], back, 0)
        return jnp.where(row8 < 8 - s, x0, x1)

    def pack(i, _):
        tiles = []
        for h in range(2):
            p = i * 16 + h * 8
            from_a = shifted(base[0] + start_a + jnp.minimum(p, seq - start_a))
            from_b = shifted(base[1] + start_b + jnp.clip(p - len_a, -8, seq - start_b))
            x = jnp.where(row8 + p < len_a, from_a, from_b)
            tiles.append(jnp.where(row8 + p < n_tok, x, 0.0))
        x = jnp.concatenate(tiles, axis=0)
        inv = lax.rsqrt(jnp.mean(x * x, axis=-1, keepdims=True) + NORM_EPS)
        u = ((x * inv) * gain_vec).astype(jnp.bfloat16)
        at = pl.ds(pl.multiple_of(i * 16, 16), 16)
        u_out[at] = u
        hp_out[at] = x.astype(jnp.bfloat16)

        @pl.when(i // (SLOTS // 32) == core)
        def _():
            half_out[pl.ds(pl.multiple_of(i * 16 - core * (SLOTS // 2), 16), 16)] = u.astype(jnp.float32)

        return 0

    lax.fori_loop(0, SLOTS // 16, pack, 0)


def _prep(hid, mask, tgt, gain):
    width = hid.shape[1]
    return pl.pallas_call(
        _prep_kernel,
        out_shape=[
            jax.ShapeDtypeStruct((SLOTS, width), jnp.bfloat16),
            jax.ShapeDtypeStruct((SLOTS // 2, width), jnp.float32),
            jax.ShapeDtypeStruct((SLOTS, width), jnp.bfloat16),
            jax.ShapeDtypeStruct((NCH, 8, CHUNK), jnp.int32),
            jax.ShapeDtypeStruct((8,), jnp.int32),
        ],
        in_specs=[VM] * 4,
        out_specs=[VM, VM, VM, VM, SM],
        scratch_shapes=[pltpu.VMEM((hid.shape[0] + 48, width), jnp.float32)],
        compiler_params=_params(),
        name="prep",
        cost_estimate=pl.CostEstimate(flops=2 * 10**9, bytes_accessed=10**7, transcendentals=0),
    )(hid, mask, tgt, gain)


def _soft(z):
    t = jnp.tanh(z * (1.0 / SOFT_CAP))
    e = jnp.exp2(t * EXP_SCALE)
    return t, e, 1.0 - t * t


def _dot_nt(a, b):
    return lax.dot_general(a, b, (((1,), (1,)), ((), ())), preferred_element_type=jnp.float32)


def _fwd_kernel(geo, meta, emb, u_ref, y_ref, q_hbm, stat_out, ebuf, qbuf, acc, esem, qsem):
    tiles, rows, brows, mrows, real_rows = geo
    width = emb.shape[1]
    vp = lax.axis_index("vp")
    row_start = vp * emb.shape[0]
    n_real = jnp.minimum(emb.shape[0], real_rows - row_start)
    n_tok = meta[4]
    nch = (n_tok + (CHUNK - 1)) // CHUNK
    for s in range(2):
        ebuf[s, rows:brows] = jnp.zeros((brows - rows, width), jnp.bfloat16)
    acc[...] = jnp.zeros_like(acc)

    def ecopy(j, s):
        return pltpu.make_async_copy(
            emb.at[pl.ds(pl.multiple_of(j * rows, 8), rows)], ebuf.at[s, pl.ds(0, rows)], esem.at[s]
        )

    def qcopy(c, j, s):
        return pltpu.make_async_copy(
            qbuf.at[s, pl.ds(0, rows)], q_hbm.at[c, pl.ds(pl.multiple_of(j * rows, 8), rows)], qsem.at[s]
        )

    ecopy(0, 0).start()
    i8 = lax.broadcasted_iota(jnp.int32, (8, CHUNK), 0)

    def tile(j, _):
        slot = lax.rem(j, 2)
        ecopy(j, slot).wait()

        @pl.when(j + 1 < tiles)
        def _():
            ecopy(j + 1, 1 - slot).start()

        hi = jnp.minimum(rows, n_real - j * rows)

        def chunk(c, _):
            k = j * nch + c
            qs = lax.rem(k, 2)

            @pl.when(k >= 2)
            def _():
                qcopy(0, 0, qs).wait()

            uc = u_ref[pl.ds(pl.multiple_of(c * CHUNK, CHUNK), CHUNK)]
            y_loc = y_ref[c] - (row_start + j * rows)
            for m in range(0, brows, mrows):
                t, e, d = _soft(_dot_nt(ebuf[slot, m : m + mrows], uc))
                if m + mrows > rows - PAD_ROWS:
                    r = lax.broadcasted_iota(jnp.int32, e.shape, 0) + m
                    e = jnp.where(r < hi, e, 0.0)
                qbuf[qs, m : m + mrows] = e * d
                s_part = [None, None]
                t_part = [jnp.zeros((8, CHUNK), jnp.float32)] * 2
                for n, g in enumerate(range(0, mrows, 8)):
                    p = n % 2
                    s_part[p] = e[g : g + 8] if s_part[p] is None else s_part[p] + e[g : g + 8]
                    t_part[p] = jnp.where(i8 + (m + g) == y_loc, t[g : g + 8], t_part[p])
                acc[0, c] += s_part[0] + s_part[1]
                acc[1, c] += t_part[0] + t_part[1]
            qcopy(c, j, qs).start()
            return 0

        lax.fori_loop(0, nch, chunk, 0)
        return 0

    lax.fori_loop(0, tiles, tile, 0)
    total = tiles * nch
    qcopy(0, 0, lax.rem(total, 2)).wait()
    qcopy(0, 0, lax.rem(total + 1, 2)).wait()
    for c in range(NCH):
        at = slice(c * CHUNK, (c + 1) * CHUNK)
        stat_out[0:1, at] = jnp.sum(acc[0, c], axis=0, keepdims=True)
        stat_out[1:2, at] = jnp.sum(acc[1, c], axis=0, keepdims=True)
        stat_out[2:3, at] = y_ref[c][0:1].astype(jnp.float32)
        stat_out[3:4, at] = jnp.full((1, CHUNK), n_tok, jnp.int32).astype(jnp.float32)


def _tiling(own_rows):
    tiles = 5
    rows = own_rows // tiles
    assert rows * tiles == own_rows and rows % 8 == 0
    brows = -(-rows // 256) * 256
    return tiles, rows, brows


def _fwd(meta, emb, u, y, real_rows):
    own, width = emb.shape
    tiles, rows, brows = _tiling(own)
    geo = (tiles, rows, brows, brows // 10, real_rows)
    return pl.pallas_call(
        functools.partial(_fwd_kernel, geo),
        out_shape=[
            jax.ShapeDtypeStruct((NCH, own, CHUNK), jnp.float32),
            jax.ShapeDtypeStruct((4, SLOTS), jnp.float32),
        ],
        in_specs=[SM, ANY, VM, VM],
        out_specs=[ANY, VM],
        scratch_shapes=[
            pltpu.VMEM((2, brows, width), jnp.bfloat16),
            pltpu.VMEM((2, brows, CHUNK), jnp.float32),
            pltpu.VMEM((2, NCH, 8, CHUNK), jnp.float32),
            pltpu.SemaphoreType.DMA((2,)),
            pltpu.SemaphoreType.DMA((2,)),
        ],
        compiler_params=_params(),
        name="fwd",
        cost_estimate=pl.CostEstimate(flops=2 * own * width * 3 * CHUNK, bytes_accessed=8 * own * width, transcendentals=0),
    )(meta, emb, u, y)


def _stats_kernel(n_dp, n_vp, stat, coef, y_out, cnt_out, loss_out, got, send, recv, lsem):
    me_d, me_v = lax.axis_index("dp"), lax.axis_index("vp")
    me = me_d * n_vp + me_v
    n = n_dp * n_vp
    barrier = pltpu.get_barrier_semaphore()
    peers = []
    for k in range(1, n):
        other = lax.rem(me + k, n)
        peers.append((other // n_vp, lax.rem(other, n_vp)))
    for p in peers:
        pl.semaphore_signal(barrier, inc=1, device_id=p, device_id_type=MESH)
    mine = pltpu.make_async_copy(stat, got.at[me], lsem)
    mine.start()
    pl.semaphore_wait(barrier, n - 1)
    copies = []
    for k, p in enumerate(peers):
        c = pltpu.make_async_remote_copy(
            src_ref=stat, dst_ref=got.at[me], send_sem=send.at[k], recv_sem=recv.at[k], device_id=p, device_id_type=MESH
        )
        c.start()
        copies.append(c)
    mine.wait()
    for c in copies:
        c.wait()
    lane = lax.broadcasted_iota(jnp.int32, (1, SLOTS), 1)
    total = jnp.zeros((1, SLOTS), jnp.float32)
    cnts = [got[d * n_vp, 3:4] for d in range(n_dp)]
    mask_count = functools.reduce(lambda a, b: a + b, cnts)
    inv_n = 1.0 / mask_count
    for d in range(n_dp):
        s = got[d * n_vp, 0:1]
        t = got[d * n_vp, 1:2]
        for v in range(1, n_vp):
            s = s + got[d * n_vp + v, 0:1]
            t = t + got[d * n_vp + v, 1:2]
        valid = lane < cnts[d].astype(jnp.int32)
        s = jnp.where(valid, s, 1.0)
        coef[d, 0] = jnp.broadcast_to(jnp.where(valid, inv_n / s, 0.0), (8, SLOTS))
        coef[d, 1] = jnp.broadcast_to(jnp.where(valid, (1.0 - t * t) * inv_n, 0.0), (8, SLOTS))
        y_out[d] = jnp.broadcast_to(got[d * n_vp, 2:3].astype(jnp.int32), (8, SLOTS))
        cnt_out[d : d + 1] = cnts[d][:, 0:128].astype(jnp.int32)
        total = total + jnp.where(valid, jnp.log(s) - SOFT_CAP * t, 0.0)
    loss_out[...] = jnp.broadcast_to(jnp.sum(total, axis=1, keepdims=True), (1, 128)) / mask_count[:, 0:128]


def _stats(stat, n_dp, n_vp):
    n = n_dp * n_vp
    return pl.pallas_call(
        functools.partial(_stats_kernel, n_dp, n_vp),
        out_shape=[
            jax.ShapeDtypeStruct((n_dp, 2, 8, SLOTS), jnp.float32),
            jax.ShapeDtypeStruct((n_dp, 8, SLOTS), jnp.int32),
            jax.ShapeDtypeStruct((n_dp, 128), jnp.int32),
            jax.ShapeDtypeStruct((1, 128), jnp.float32),
        ],
        in_specs=[VM],
        out_specs=[VM] * 4,
        scratch_shapes=[
            pltpu.VMEM((n, 4, SLOTS), jnp.float32),
            pltpu.SemaphoreType.DMA((n - 1,)),
            pltpu.SemaphoreType.DMA((n - 1,)),
            pltpu.SemaphoreType.DMA,
        ],
        compiler_params=_params(collective_id=0, has_side_effects=True),
        name="stats",
        cost_estimate=pl.CostEstimate(flops=2 * 10**9, bytes_accessed=10**6, transcendentals=0),
    )(stat)


def _mid_kernel(
    geo, cnt, emb, q_hbm, ua, ub, hp, coef, y_ref, g_hbm, du_out, uo_out, ebuf, qbuf, gown, goth, ustage, esem, qsem, osem, psem, usem
):
    tiles, rows, brows, mrows, real_rows = geo
    width = emb.shape[1]
    me_d, vp = lax.axis_index("dp"), lax.axis_index("vp")
    core = lax.rem(vp, 2)
    ot_d = 1 - me_d
    row_start = vp * emb.shape[0]
    n_real = jnp.minimum(emb.shape[0], real_rows - row_start)
    n_own = (cnt[me_d, 0] + (CHUNK - 1)) // CHUNK
    n_oth = (cnt[ot_d, 0] + (CHUNK - 1)) // CHUNK

    def ecopy(j, s):
        return pltpu.make_async_copy(
            emb.at[pl.ds(pl.multiple_of(j * rows, 8), rows)], ebuf.at[s, pl.ds(0, rows)], esem.at[s]
        )

    def qcopy(c, j, s):
        return pltpu.make_async_copy(
            q_hbm.at[c, pl.ds(pl.multiple_of(j * rows, 8), rows)], qbuf.at[s, pl.ds(0, rows)], qsem.at[s]
        )

    def gcopy(buf, sem, d, c, j, s):
        return pltpu.make_async_copy(
            buf.at[s, pl.ds(0, rows)], g_hbm.at[d, c, pl.ds(pl.multiple_of(j * rows, 8), rows)], sem.at[s]
        )

    ecopy(0, 0).start()
    qcopy(0, 0, 0).start()
    half = SLOTS // 2
    for n, src in enumerate((ua, ub)):
        cp = pltpu.make_async_copy(src, ustage, usem)
        cp.start()
        cp.wait()
        at = core if n == 0 else 1 - core
        uo_out[pl.ds(pl.multiple_of(at * half, half), half)] = ustage[...].astype(jnp.bfloat16)
    for s in range(2):
        ebuf[s, rows:brows] = jnp.zeros((brows - rows, width), jnp.bfloat16)
        qbuf[s, rows:brows] = jnp.zeros((brows - rows, CHUNK), jnp.float32)
    du_out[...] = jnp.zeros_like(du_out)

    def tile(j, _):
        slot = lax.rem(j, 2)
        ecopy(j, slot).wait()

        @pl.when(j + 1 < tiles)
        def _():
            ecopy(j + 1, 1 - slot).start()

        hi = jnp.minimum(rows, n_real - j * rows)

        def own(c, _):
            k = j * n_own + c
            s = lax.rem(k, 2)
            qcopy(c, j, s).wait()

            @pl.when(k + 1 < tiles * n_own)
            def _():
                last = c + 1 == n_own
                qcopy(jnp.where(last, 0, c + 1), jnp.where(last, j + 1, j), 1 - s).start()

            @pl.when(k >= 2)
            def _():
                gcopy(gown, osem, 0, 0, 0, s).wait()

            at = pl.ds(pl.multiple_of(c * CHUNK, CHUNK), CHUNK)
            y_loc = y_ref[me_d, :, at] - (row_start + j * rows)
            scale = coef[me_d, 0, 0:1, at]
            hit_w = coef[me_d, 1, 0:1, at]
            for m in range(0, brows, mrows):
                r = lax.broadcasted_iota(jnp.int32, (mrows, CHUNK), 0) + m
                g = qbuf[s, m : m + mrows] * scale - jnp.where(r == y_loc[0:1], hit_w, 0.0)
                if m + mrows > rows:
                    g = jnp.where(r < rows, g, 0.0)
                gown[s, m : m + mrows] = g.astype(jnp.bfloat16)
            du_out[at] += lax.dot_general(
                gown[s], ebuf[slot], (((0,), (0,)), ((), ())), preferred_element_type=jnp.float32
            )
            gcopy(gown, osem, me_d, c, j, s).start()
            return 0

        lax.fori_loop(0, n_own, own, 0)

        def other(c, _):
            k = j * n_oth + c
            s = lax.rem(k, 2)

            @pl.when(k >= 2)
            def _():
                gcopy(goth, psem, 0, 0, 0, s).wait()

            at = pl.ds(pl.multiple_of(c * CHUNK, CHUNK), CHUNK)
            uc = uo_out[at]
            y_loc = y_ref[ot_d, :, at] - (row_start + j * rows)
            scale = coef[ot_d, 0, 0:1, at]
            hit_w = coef[ot_d, 1, 0:1, at]
            for m in range(0, brows, mrows):
                _, e, d = _soft(_dot_nt(ebuf[slot, m : m + mrows], uc))
                r = lax.broadcasted_iota(jnp.int32, e.shape, 0) + m
                if m + mrows > rows - PAD_ROWS:
                    e = jnp.where(r < hi, e, 0.0)
                g = (e * d) * scale - jnp.where(r == y_loc[0:1], hit_w, 0.0)
                goth[s, m : m + mrows] = g.astype(jnp.bfloat16)
            gcopy(goth, psem, ot_d, c, j, s).start()
            return 0

        lax.fori_loop(0, n_oth, other, 0)
        return 0

    lax.fori_loop(0, tiles, tile, 0)
    for buf, sem, n in ((gown, osem, n_own), (goth, psem, n_oth)):
        total = tiles * n
        gcopy(buf, sem, 0, 0, 0, lax.rem(total, 2)).wait()
        gcopy(buf, sem, 0, 0, 0, lax.rem(total + 1, 2)).wait()

    def gain_part(i, acc):
        at = pl.ds(pl.multiple_of(i * 64, 64), 64)
        x = hp[at].astype(jnp.float32)
        inv = lax.rsqrt(jnp.mean(x * x, axis=-1, keepdims=True) + NORM_EPS)
        v = du_out[at] * (x * inv)
        for g in range(0, 64, 8):
            acc = acc + v[g : g + 8]
        return acc

    acc = lax.fori_loop(0, SLOTS // 64, gain_part, jnp.zeros((8, width), jnp.float32))
    du_out[SLOTS : SLOTS + 8] = acc


def _mid(cnt, emb, q, ua, ub, hp, coef, y, real_rows):
    own, width = emb.shape
    tiles, rows, brows = _tiling(own)
    geo = (tiles, rows, brows, brows // 10, real_rows)
    return pl.pallas_call(
        functools.partial(_mid_kernel, geo),
        out_shape=[
            jax.ShapeDtypeStruct((2, NCH, own, CHUNK), jnp.bfloat16),
            jax.ShapeDtypeStruct((SLOTS + 8, width), jnp.float32),
            jax.ShapeDtypeStruct((SLOTS, width), jnp.bfloat16),
        ],
        in_specs=[SM, ANY, ANY, ANY, ANY, VM, VM, VM],
        out_specs=[ANY, VM, VM],
        scratch_shapes=[
            pltpu.VMEM((2, brows, width), jnp.bfloat16),
            pltpu.VMEM((2, brows, CHUNK), jnp.float32),
            pltpu.VMEM((2, brows, CHUNK), jnp.bfloat16),
            pltpu.VMEM((2, brows, CHUNK), jnp.bfloat16),
            pltpu.VMEM((SLOTS // 2, width), jnp.float32),
        ]
        + [pltpu.SemaphoreType.DMA((2,))] * 4
        + [pltpu.SemaphoreType.DMA],
        compiler_params=_params(),
        name="mid",
        cost_estimate=pl.CostEstimate(flops=4 * own * width * 3 * CHUNK, bytes_accessed=8 * own * width, transcendentals=0),
    )(cnt, emb, q, ua, ub, hp, coef, y)


def _table_kernel(geo, cnt, g_hbm, u_own, u_oth, out, uall, gbuf, obuf, gsem, osem, usem):
    tiles, rows = geo
    me_d = lax.axis_index("dp")
    n0 = (cnt[0, 0] + (CHUNK - 1)) // CHUNK
    n1 = (cnt[1, 0] + (CHUNK - 1)) // CHUNK
    n = n0 + n1

    def where(i):
        d = jnp.where(i < n0, 0, 1)
        return d, i - d * n0

    def gcopy(i, j, s):
        d, c = where(i)
        return pltpu.make_async_copy(
            g_hbm.at[d, c, pl.ds(pl.multiple_of(j * rows, 8), rows)], gbuf.at[s, i], gsem.at[s]
        )

    def gstart(j, s):
        lax.fori_loop(0, n, lambda i, _: (gcopy(i, j, s).start(), 0)[1], 0)

    def gwait(j, s):
        lax.fori_loop(0, n, lambda i, _: (gcopy(i, j, s).wait(), 0)[1], 0)

    def ocopy(j, s):
        return pltpu.make_async_copy(obuf.at[s], out.at[pl.ds(pl.multiple_of(j * rows, 8), rows)], osem.at[s])

    gstart(0, 0)
    cps = [
        pltpu.make_async_copy(u_own, uall.at[me_d], usem.at[0]),
        pltpu.make_async_copy(u_oth, uall.at[1 - me_d], usem.at[1]),
    ]
    for cp in cps:
        cp.start()
    for cp in cps:
        cp.wait()

    def tile(j, _):
        s = lax.rem(j, 2)
        gwait(j, s)

        @pl.when(j + 1 < tiles)
        def _():
            gstart(j + 1, 1 - s)

        @pl.when(j >= 2)
        def _():
            ocopy(j, s).wait()

        def part(i):
            d, c = where(i)
            uc = uall[d, pl.ds(pl.multiple_of(c * CHUNK, CHUNK), CHUNK)]
            return jnp.dot(gbuf[s, i], uc, preferred_element_type=jnp.float32)

        obuf[s] = part(0)

        def more(i, _):
            obuf[s] += part(i)
            return 0

        lax.fori_loop(1, n, more, 0)
        ocopy(j, s).start()
        return 0

    lax.fori_loop(0, tiles, tile, 0)
    ocopy(0, 0).wait()
    ocopy(0, 1).wait()


def _table(cnt, g, u_own, u_oth):
    own, width = g.shape[2], u_own.shape[1]
    tiles = 19
    rows = own // tiles
    assert rows * tiles == own and rows % 8 == 0
    return pl.pallas_call(
        functools.partial(_table_kernel, (tiles, rows)),
        out_shape=jax.ShapeDtypeStruct((own, width), jnp.float32),
        in_specs=[SM, ANY, ANY, ANY],
        out_specs=ANY,
        scratch_shapes=[
            pltpu.VMEM((2, SLOTS, width), jnp.bfloat16),
            pltpu.VMEM((2, 2 * NCH, rows, CHUNK), jnp.bfloat16),
            pltpu.VMEM((2, rows, width), jnp.float32),
            pltpu.SemaphoreType.DMA((2,)),
            pltpu.SemaphoreType.DMA((2,)),
            pltpu.SemaphoreType.DMA((2,)),
        ],
        compiler_params=_params(),
        name="table",
        cost_estimate=pl.CostEstimate(flops=2 * own * width * 5 * CHUNK, bytes_accessed=8 * own * width, transcendentals=0),
    )(cnt, g, u_own, u_oth)


def _final_kernel(meta, hid, du, gain, out, dus):
    seq, width = hid.shape[0] // 2, hid.shape[1]
    gain_vec = 1.0 + gain[...]
    pad = 8
    dus[0:pad] = jnp.zeros((pad, width), jnp.float32)
    dus[pad : pad + SLOTS] = du[0:SLOTS]
    dus[pad + SLOTS : 2 * pad + SLOTS] = jnp.zeros((pad, width), jnp.float32)
    row8 = lax.broadcasted_iota(jnp.int32, (8, width), 0)
    for smp in range(2):
        start, length = meta[2 * smp], meta[2 * smp + 1]
        base = meta[1] if smp else 0

        def block(i, _, smp=smp, start=start, length=length, base=base):
            at = pl.ds(pl.multiple_of(smp * seq + i * 16, 16), 16)
            live = (i * 16 + 16 > start) & (i * 16 < start + length)

            @pl.when(jnp.logical_not(live))
            def _():
                out[at] = jnp.zeros((16, width), jnp.float32)

            @pl.when(live)
            def _():
                x16 = hid[at].astype(jnp.float32)
                for h in range(2):
                    first = i * 16 + h * 8
                    p = jnp.clip(first - start, -8, length) + base + pad
                    lo = pl.multiple_of((p // 8) * 8, 8)
                    s = p - lo
                    back = lax.rem(8 - s, 8)
                    x0 = pltpu.roll(dus[pl.ds(lo, 8)], back, 0)
                    x1 = pltpu.roll(dus[pl.ds(jnp.minimum(lo + 8, SLOTS + pad), 8)], back, 0)
                    d8 = jnp.where(row8 < 8 - s, x0, x1)
                    tok = row8 + first
                    d8 = jnp.where((tok >= start) & (tok < start + length), d8, 0.0)
                    x = x16[h * 8 : h * 8 + 8]
                    inv = lax.rsqrt(jnp.mean(x * x, axis=-1, keepdims=True) + NORM_EPS)
                    a = d8 * gain_vec
                    dot = jnp.mean(a * x, axis=-1, keepdims=True)
                    out[pl.ds(pl.multiple_of(smp * seq + first, 8), 8)] = inv * a - x * (inv * inv * inv) * dot

            return 0

        lax.fori_loop(0, seq // 16, block, 0)


def _final(meta, hid, du, gain):
    width = hid.shape[1]
    return pl.pallas_call(
        _final_kernel,
        out_shape=jax.ShapeDtypeStruct(hid.shape, jnp.float32),
        in_specs=[SM, VM, VM, VM],
        out_specs=VM,
        scratch_shapes=[pltpu.VMEM((SLOTS + 16, width), jnp.float32)],
        compiler_params=_params(),
        name="final",
        cost_estimate=pl.CostEstimate(flops=2 * 10**9, bytes_accessed=10**7, transcendentals=0),
    )(meta, hid, du, gain)


def solution(mesh):
    n_dp, n_vp = mesh.shape["dp"], mesh.shape["vp"]

    def shard_fn(hidden, targets, loss_mask, norm_gain, emb_table):
        samples, seq_len, width = hidden.shape
        real_rows = emb_table.shape[0] * n_vp - PAD_ROWS
        hid = hidden.reshape(samples * seq_len, width)
        gain = norm_gain.reshape(1, width)
        u_own, u_half, h_pack, y_pack, meta = _prep(hid, loss_mask, targets, gain)
        far = lax.ppermute(u_half, "dp", [(i, 1 - i) for i in range(n_dp)])
        q, stat = _fwd(meta, emb_table, u_own, y_pack, real_rows)
        far, stat = lax.optimization_barrier((far, stat))
        near = lax.ppermute(far, "vp", [(i, i ^ 1) for i in range(n_vp)])
        coef, y_all, cnt, loss = _stats(stat, n_dp, n_vp)
        g, du, u_oth = _mid(cnt, emb_table, q, far, near, h_pack, coef, y_all, real_rows)
        du = lax.psum(du, "vp")
        table_grad = _table(cnt, g, u_own, u_oth)
        du, table_grad = lax.optimization_barrier((du, table_grad))
        dg = jnp.sum(du[SLOTS:], axis=0)
        dg_far = lax.ppermute(dg, "dp", [(i, 1 - i) for i in range(n_dp)])
        hid_grad = _final(meta, hid, du, gain)
        return loss[0, 0], hid_grad.reshape(hidden.shape), table_grad, dg + dg_far

    return jax.shard_map(
        shard_fn,
        mesh=mesh,
        in_specs=(P("dp"), P("dp"), P("dp"), P(), P("vp")),
        out_specs=(P(), P("dp"), P("vp"), P()),
        check_vma=False,
    )
```
